32 devices in a mesh: section: 4 (over y, core), dp: 2 (over x), expert: 4 (over z).
Axes of the slice: x: 2, y: 2, z: 4, core: 2. Of those that a mesh axis runs over, the one named last changes fastest.
Arguments:
- inputs: bfloat16 [4, 1024, 2048], P('section', ('dp', 'expert')), may hold values from -6 to 6
- in_cache: bfloat16 [4, 1024, 2048], P('section', ('dp', 'expert')), may hold values from -6 to 6
- out_cache: bfloat16 [4, 1024, 2048], P('section', ('dp', 'expert')), may hold values from -6 to 6
- w_up: bfloat16 [4, 2048, 57344], P('section', None, ('dp', 'expert')), may hold values from -0.125 to 0.125
- w_down: bfloat16 [4, 57344, 2048], P('section', ('dp', 'expert')), may hold values from -0.0625 to 0.0625
- routing: int32 [4, 1024, 2], P('section', ('dp', 'expert')), may hold values from 0 to 7, all different within a row; in each aligned block of 128 rows (0 to 127, 128 to 255, ..., all dimensions but the last counted through in order) at most 32 rows name the same one
- gate_table: int32 [4, 1024, 2], P('section', ('dp', 'expert')), may hold values from 1 to 16
- lengths: int32 [64], P(('dp', 'expert')), may hold values from 1 to 16
- sample_map: int32 [64], replicated, may hold values from 0 to 63, as said below
Outputs:
- next_input: bfloat16 [4, 1024, 2048], P('section', ('dp', 'expert'))
- new_out_cache: bfloat16 [4, 1024, 2048], P('section', ('dp', 'expert'))
The draws below stay inside these ranges and needn't reach their ends.
Inputs may be any that keep to these rules, and one draw needn't show every extreme that they name: `sample_map`: A permutation. Every sample keeps its index along expert; the samples of one device go to exactly 2 replicas, exactly 4 to each. `routing`: A row names 2 different experts; in the rows of one device each expert is named exactly 32 times.
All inputs are finite; a program needn't handle non-finite values.
Results may differ from the reference program's by a relative error of at most 0.007.
Values may be sent and summed in bfloat16 or wider, within the bound.
A program may use at most 128 MiB of HBM per device.

```python
import math
import jax
import jax.numpy as jnp
import numpy as np
from jax import lax

D = 2048
FF = 7168
EXPERTS = 8
TOPK = 2
ROWS = 16
SAMP_DEV = 8
TOK_DEV = 128
SAMPLES = 64
TOKENS = 1024
CAP_E = 32
CAP_S = 4
N_SECTION = 4
N_DP = 2
N_EXPERT = 4


def shuffled_rows(row_key, count, length):
    return jax.vmap(lambda single_key: jax.random.permutation(single_key, length))(jax.random.split(row_key, count))


def draw_sample_map(key, part):
    block_count = SAMP_DEV // CAP_S
    columns = []
    for column in range(N_EXPERT):
        column_key = jax.random.fold_in(key, 101 + column)
        outer_perm = jax.random.permutation(jax.random.fold_in(column_key, 1), N_DP)
        inner_perm = jax.random.permutation(jax.random.fold_in(column_key, 2), N_DP)
        offsets = jax.random.permutation(jax.random.fold_in(column_key, 3), N_DP)[:block_count]
        turned = shuffled_rows(jax.random.fold_in(column_key, 4), N_DP, SAMP_DEV)
        settle = shuffled_rows(jax.random.fold_in(column_key, 5), N_DP, SAMP_DEV)
        block_ids = turned // CAP_S
        within = turned % CAP_S
        dest_rep = outer_perm[(inner_perm[:, None] + offsets[block_ids]) % N_DP]
        new_local = settle[dest_rep, block_ids * CAP_S + within]
        columns.append((dest_rep * N_EXPERT + column) * SAMP_DEV + new_local)
    stacked = jnp.stack(columns, axis=1)
    return stacked.reshape(SAMPLES).astype(jnp.int32)


def plant(array, stream_key, smallest, largest):
    shape = array.shape
    index_at = [jax.random.randint(jax.random.fold_in(stream_key, axis), (), 0, shape[axis]) for axis in range(len(shape))]
    array = array.at[tuple(index_at)].set(smallest)
    longest = shape.index(max(shape))
    index_at[longest] = (index_at[longest] + 1) % shape[longest]
    return array.at[tuple(index_at)].set(largest)


def block_levels(key, dims, cuts, low, top_value):
    factor_of = 1.0
    for dim, shards_of in cuts:
        draws = jax.random.uniform(jax.random.fold_in(jax.random.fold_in(key, 6), dim), (shards_of,), jnp.float32, low / len(cuts), top_value / len(cuts))
        factor_of = factor_of * jnp.repeat(jnp.exp(draws), dims[dim] // shards_of).reshape((-1,) + (1,) * (len(dims) - 1 - dim))
    return factor_of


def routed_block(own_key, own, number, rows, count, top, most, slope):
    sequence = jax.random.permutation(own_key, count)
    heavy_load, ordinary = shares(count, rows * top, most, slope, True), shares(count, rows * top, most, slope, False)
    places = jnp.arange(count)

    def named(sizes, offset_by):
        used = int((sizes > 0).sum())
        fixed = max(1, used // 4)
        passed = fixed + (places - fixed + offset_by * (used - fixed)) % max(1, count - fixed)
        return jnp.zeros((count,), jnp.int32).at[sequence[jnp.where(places < fixed, places, passed)]].set(jnp.asarray(sizes, jnp.int32))

    sizes = jnp.where(number % 4 == 0, named(heavy_load, number // 4), named(ordinary, number - number // 4 - 1))
    mixed = jax.random.permutation(jax.random.fold_in(own, 3), count)
    donor, sink = mixed[0:count // 2 * 2:2], mixed[1:count // 2 * 2:2]
    slack = jnp.minimum(sizes[donor] - 1, most - sizes[sink]) // 2
    slack = jnp.where((donor == sequence[0]) | (sink == sequence[0]) | (sizes[sink] == 0), 0, jnp.maximum(slack, 0))
    passed = jax.random.randint(jax.random.fold_in(own, 4), (count // 2,), 0, 1 << 20) % (slack + 1)
    sizes = sizes.at[donor].add(-passed).at[sink].add(passed)
    items = jnp.searchsorted(jnp.cumsum(sizes), jnp.arange(rows * top), side="right").astype(jnp.int32)
    listing = items.reshape(top, rows).T
    listing = listing[jax.random.permutation(jax.random.fold_in(own, 1), rows)]
    offset_by = jax.random.randint(jax.random.fold_in(own, 2), (rows, 1), 0, top)
    return jnp.take_along_axis(listing, (jnp.arange(top)[None, :] + offset_by) % top, axis=1)


def shares(number_of, total, most, skew, full):
    loads = [(1 << 20) // math.isqrt(grade ** skew) + 1 for grade in range(1, number_of + 1)]
    largest = most if full else min(most, max(-(-total // number_of), total * loads[0] // sum(loads)))
    least = 1 if total - largest >= number_of - 1 else 0
    holding, surplus = [largest] + [least] * (number_of - 1), total - largest - least * (number_of - 1)
    while surplus > 0:
        free = [i for i in range(1, number_of) if holding[i] < largest] or [i for i in range(1, number_of) if holding[i] < most]
        mass, remaining = sum([loads[i] for i in free]), surplus
        for i in free:
            more = min(most - holding[i], max(1, remaining * loads[i] // mass), surplus)
            holding[i] = holding[i] + more
            surplus = surplus - more
    return np.array(holding)


def scatter_about(own_key, dims, scale, most, cuts=(), held_as=jnp.bfloat16):
    result = scale * jax.random.normal(own_key, dims, jnp.float32)
    if cuts:
        result = result * block_levels(own_key, dims, cuts, -0.22, 0.18)
    return jnp.clip(result, -most, most).astype(held_as)


def setup_inputs(seed: int = 0) -> dict:
    key_of = jax.random.split(jax.random.key(seed), 10)
    inputs = scatter_about(key_of[0], (N_SECTION, TOKENS, D), 1.0, 6.0, ((0, 4), (1, 8)))
    in_cache = scatter_about(key_of[1], (N_SECTION, TOKENS, D), 1.0, 6.0, ((0, 4), (1, 8)))
    out_cache = scatter_about(key_of[2], (N_SECTION, TOKENS, D), 1.0, 6.0, ((0, 4), (1, 8)))
    w_up = scatter_about(key_of[3], (N_SECTION, D, EXPERTS * FF), D ** -0.5, 0.125, ((0, 4), (2, 8)))
    w_down = scatter_about(key_of[4], (N_SECTION, EXPERTS * FF, D), FF ** -0.5, 0.0625, ((0, 4), (1, 8)))
    routing_keys = jax.random.split(jax.random.fold_in(key_of[5], 1), N_SECTION * TOKENS // TOK_DEV)
    routing_turns = jax.random.permutation(jax.random.fold_in(key_of[5], 3), N_SECTION * TOKENS // TOK_DEV)
    routing = jax.vmap(lambda own, number: routed_block(jax.random.fold_in(key_of[5], 2), own, number, TOK_DEV, EXPERTS, TOPK, CAP_E, 0))(routing_keys, routing_turns).reshape((N_SECTION, TOKENS, TOPK))
    gate_table = plant(jax.random.randint(key_of[6], (N_SECTION, TOKENS, TOPK), 1, 17), jax.random.fold_in(key_of[6], 1), 1, 16).astype(jnp.int32)
    lengths = plant(jax.random.randint(key_of[7], (SAMPLES,), 1, ROWS + 1), jax.random.fold_in(key_of[7], 1), 1, ROWS).astype(jnp.int32)
    sample_map = draw_sample_map(jax.random.fold_in(key_of[9], 71), 0)
    return dict(inputs=inputs, in_cache=in_cache, out_cache=out_cache, w_up=w_up, w_down=w_down, routing=routing, gate_table=gate_table, lengths=lengths, sample_map=sample_map)


def reference(inputs, in_cache, out_cache, w_up, w_down, routing, gate_table, lengths, sample_map):
    feature_width = inputs.shape[2]
    total_samples = sample_map.shape[0]
    sources = jnp.zeros((total_samples,), jnp.int32).at[sample_map].set(jnp.arange(total_samples, dtype=jnp.int32))

    def migrate(cache):
        shaped = cache.reshape(N_SECTION, total_samples, ROWS, feature_width)
        return shaped[:, sources].reshape(N_SECTION, total_samples * ROWS, feature_width)

    in_moved = migrate(in_cache)
    out_moved = migrate(out_cache)
    slice_count = N_DP * N_EXPERT // EXPERTS
    slice_width = FF // slice_count
    per_expert = total_samples * ROWS * TOPK // EXPERTS

    def expert_layer(section_args):
        tokens, up_section, down_section, chosen, gates = section_args
        flat_experts = chosen.reshape(-1)
        sorted_order = jnp.argsort(flat_experts, stable=True).astype(jnp.int32)
        grouped = tokens[sorted_order // TOPK].reshape(EXPERTS, per_expert, feature_width)
        up_all = up_section.reshape(feature_width, EXPERTS, FF).transpose(1, 0, 2)
        down_all = down_section.reshape(EXPERTS, FF, feature_width)

        def one_expert(expert_args):
            rows_here, up_here, down_here = expert_args
            hidden = jax.nn.silu(jnp.dot(rows_here, up_here, preferred_element_type=jnp.float32)).astype(jnp.bfloat16)
            pieces = jnp.einsum("rsf,sfd->srd",
                                hidden.reshape(per_expert, slice_count, slice_width).astype(jnp.float32),
                                down_here.reshape(slice_count, slice_width, feature_width).astype(jnp.float32))
            rounded = lax.optimization_barrier(pieces.astype(jnp.bfloat16)).astype(jnp.float32)
            return jnp.sum(rounded, axis=0)

        expert_rows = lax.map(one_expert, (grouped, up_all, down_all)).reshape(-1, feature_width)
        position = jnp.zeros_like(sorted_order).at[sorted_order].set(jnp.arange(sorted_order.shape[0], dtype=jnp.int32))
        per_assign = expert_rows[position].reshape(tokens.shape[0], TOPK, feature_width)
        weights = gates.astype(jnp.float32)
        weights = weights / jnp.sum(weights, axis=1, keepdims=True)
        return jnp.sum(weights[:, :, None] * per_assign, axis=1)

    mixed = lax.map(expert_layer, (inputs, w_up, w_down, routing, gate_table))
    valid_rows = (jnp.arange(ROWS, dtype=jnp.int32)[None, :] < lengths[:, None]).reshape(-1)
    delta_rows = jnp.where(valid_rows[None, :, None], (mixed - out_moved.astype(jnp.float32)).astype(jnp.bfloat16), jnp.zeros((), jnp.bfloat16))
    new_out_cache = (out_moved.astype(jnp.float32) + delta_rows.astype(jnp.float32)).astype(jnp.bfloat16)
    received = jnp.concatenate([jnp.zeros_like(delta_rows[:1]), delta_rows[:-1]], axis=0)
    next_input = (in_moved.astype(jnp.float32) + received.astype(jnp.float32)).astype(jnp.bfloat16)
    return next_input, new_out_cache
```

```python
import jax
import jax.numpy as jnp
from jax import lax
from jax.sharding import PartitionSpec as P

EXPERTS = 8
TOPK = 2
ROWS = 16
SAMP_DEV = 8


def from_behind(value, axis, by):
    peers = lax.axis_size(axis)
    pairs = [(i, i + by) for i in range(peers) if 0 <= i + by < peers]
    return lax.ppermute(value, axis, pairs)


def cache_plan(sample_map, own_device, own_dp, dp_count, expert_count, cap_slots):
    total = sample_map.shape[0]
    ids = jnp.arange(total, dtype=jnp.int32)
    local = jnp.arange(SAMP_DEV, dtype=jnp.int32)
    own_map = lax.dynamic_slice_in_dim(sample_map, own_device * SAMP_DEV, SAMP_DEV)
    dest_dp = own_map // (SAMP_DEV * expert_count)
    slot = jnp.sum(
        ((dest_dp[:, None] == dest_dp[None, :]) & (local[None, :] < local[:, None])).astype(jnp.int32),
        axis=1,
    )
    places = jnp.arange(dp_count * cap_slots, dtype=jnp.int32)
    to_send = jnp.sum(
        jnp.where(places[:, None] == (dest_dp * cap_slots + slot)[None, :], local[None, :], 0), axis=1
    )
    wanted = own_device * SAMP_DEV + local
    sources = jnp.sum(jnp.where(sample_map[None, :] == wanted[:, None], ids[None, :], 0), axis=1)
    source_device = sources // SAMP_DEV
    earlier = (
        (ids[None, :] // SAMP_DEV == source_device[:, None])
        & (ids[None, :] < sources[:, None])
        & (sample_map[None, :] // (SAMP_DEV * expert_count) == own_dp)
    )
    arrival = source_device // expert_count * cap_slots + jnp.sum(earlier.astype(jnp.int32), axis=1)
    return to_send, arrival


def token_plan(routing, gate_table, per_expert):
    tok_rows = routing.shape[0]
    before = jnp.arange(tok_rows)[None, :] < jnp.arange(tok_rows)[:, None]
    weights = gate_table.astype(jnp.float32)
    weights = weights / jnp.sum(weights, axis=1, keepdims=True)
    slots = jnp.arange(EXPERTS * per_expert, dtype=jnp.int32)
    select, mix = 0, 0
    for k in range(TOPK):
        own = routing[:, k]
        rank = 0
        for j in range(TOPK):
            rank = rank + jnp.sum((before & (routing[:, j][None, :] == own[:, None])).astype(jnp.int32), axis=1)
        slot = own * per_expert + rank
        select = select + (slots[:, None] == slot[None, :]).astype(jnp.bfloat16)
        mix = mix + jnp.where(slots[None, :] == slot[:, None], weights[:, k][:, None], 0.0)
    return select, mix


def per_device(inputs, in_cache, out_cache, w_up, w_down, routing, gate_table, lengths, sample_map):
    tok_rows, width = inputs.shape[1:]
    dp_count = lax.axis_size("dp")
    expert_count = lax.axis_size("expert")
    group_size = dp_count * expert_count
    slice_count = group_size // EXPERTS
    own_dp = lax.axis_index("dp")
    own_device = own_dp * expert_count + lax.axis_index("expert")
    cap_slots = max(1, SAMP_DEV // dp_count)
    per_expert = tok_rows * TOPK // EXPERTS

    select, mix = token_plan(routing[0], gate_table[0], per_expert)
    grouped = jnp.dot(select, inputs[0], preferred_element_type=jnp.float32).astype(jnp.bfloat16)
    grouped = grouped.reshape(EXPERTS, 1, per_expert, width)
    outgoing = jnp.broadcast_to(grouped, (EXPERTS, slice_count, per_expert, width)).reshape(
        group_size, per_expert, width
    )
    arrived = lax.all_to_all(outgoing, ("dp", "expert"), split_axis=0, concat_axis=0, tiled=True)

    to_send, arrival = cache_plan(sample_map, own_device, own_dp, dp_count, expert_count, cap_slots)
    send = jnp.concatenate(
        [
            in_cache[0].reshape(SAMP_DEV, 1, ROWS, width)[to_send],
            out_cache[0].reshape(SAMP_DEV, 1, ROWS, width)[to_send],
        ],
        axis=1,
    )
    send, arrived = lax.optimization_barrier((send, arrived))
    got = lax.all_to_all(send, "dp", split_axis=0, concat_axis=0, tiled=True)

    hidden = jax.nn.silu(
        jnp.dot(arrived.reshape(-1, width), w_up[0], preferred_element_type=jnp.float32)
    ).astype(jnp.bfloat16)
    partial_value = jnp.dot(hidden, w_down[0], preferred_element_type=jnp.float32).astype(jnp.bfloat16)
    returned = lax.all_to_all(
        partial_value.reshape(arrived.shape), ("dp", "expert"), split_axis=0, concat_axis=0, tiled=True
    ).reshape(-1, width)

    mix = jnp.broadcast_to(
        mix.reshape(tok_rows, EXPERTS, 1, per_expert), (tok_rows, EXPERTS, slice_count, per_expert)
    ).reshape(tok_rows, -1)
    high = mix.astype(jnp.bfloat16)
    low = (mix - high.astype(jnp.float32)).astype(jnp.bfloat16)
    both = jnp.dot(jnp.concatenate([high, low], axis=0), returned, preferred_element_type=jnp.float32)
    mixed = both[:tok_rows] + both[tok_rows:]

    in_moved = got[arrival, 0].reshape(tok_rows, width)
    out_moved = got[arrival, 1].reshape(tok_rows, width)
    row_numbers = jnp.arange(tok_rows, dtype=jnp.int32) % ROWS
    valid_rows = row_numbers < jnp.repeat(lengths, ROWS)
    delta_rows = jnp.where(
        valid_rows[:, None],
        (mixed - out_moved.astype(jnp.float32)).astype(jnp.bfloat16),
        jnp.zeros((), jnp.bfloat16),
    )
    new_out = (out_moved.astype(jnp.float32) + delta_rows.astype(jnp.float32)).astype(jnp.bfloat16)
    received = from_behind(delta_rows, "section", 1)
    next_input = (in_moved.astype(jnp.float32) + received.astype(jnp.float32)).astype(jnp.bfloat16)
    return (next_input[None], new_out[None])


def solution(mesh):
    split = P("section", ("dp", "expert"), None)
    placed = (split, split, split, P("section", None, ("dp", "expert")), split, split, split, P(("dp", "expert")), P())
    return jax.shard_map(per_device, mesh=mesh, in_specs=placed, out_specs=(split, split), check_vma=False)
```

```python
import functools

import jax
import jax.numpy as jnp
from jax import lax
from jax.experimental import pallas as pl
from jax.experimental.pallas import tpu as pltpu
from jax.sharding import PartitionSpec as P

EXPERTS = 8
TOPK = 2
ROWS = 16
SAMP_DEV = 8


def from_behind(value, axis, by):
    peers = lax.axis_size(axis)
    pairs = [(i, i + by) for i in range(peers) if 0 <= i + by < peers]
    return lax.ppermute(value, axis, pairs)


def cache_plan(sample_map, own_device, own_dp, dp_count, expert_count, cap_slots):
    total = sample_map.shape[0]
    ids = jnp.arange(total, dtype=jnp.int32)
    local = jnp.arange(SAMP_DEV, dtype=jnp.int32)
    own_map = lax.dynamic_slice_in_dim(sample_map, own_device * SAMP_DEV, SAMP_DEV)
    dest_dp = own_map // (SAMP_DEV * expert_count)
    slot = jnp.sum(
        ((dest_dp[:, None] == dest_dp[None, :]) & (local[None, :] < local[:, None])).astype(jnp.int32),
        axis=1,
    )
    places = jnp.arange(dp_count * cap_slots, dtype=jnp.int32)
    to_send = jnp.sum(
        jnp.where(places[:, None] == (dest_dp * cap_slots + slot)[None, :], local[None, :], 0), axis=1
    )
    wanted = own_device * SAMP_DEV + local
    sources = jnp.sum(jnp.where(sample_map[None, :] == wanted[:, None], ids[None, :], 0), axis=1)
    source_device = sources // SAMP_DEV
    earlier = (
        (ids[None, :] // SAMP_DEV == source_device[:, None])
        & (ids[None, :] < sources[:, None])
        & (sample_map[None, :] // (SAMP_DEV * expert_count) == own_dp)
    )
    arrival = source_device // expert_count * cap_slots + jnp.sum(earlier.astype(jnp.int32), axis=1)
    return to_send, arrival


def token_plan(routing, gate_table, per_expert):
    tok_rows = routing.shape[0]
    before = jnp.arange(tok_rows)[None, :] < jnp.arange(tok_rows)[:, None]
    weights = gate_table.astype(jnp.float32)
    weights = weights / jnp.sum(weights, axis=1, keepdims=True)
    slots = jnp.arange(EXPERTS * per_expert, dtype=jnp.int32)
    select, mix = 0, 0
    for k in range(TOPK):
        own = routing[:, k]
        rank = 0
        for j in range(TOPK):
            rank = rank + jnp.sum((before & (routing[:, j][None, :] == own[:, None])).astype(jnp.int32), axis=1)
        slot = own * per_expert + rank
        select = select + (slots[:, None] == slot[None, :]).astype(jnp.bfloat16)
        mix = mix + jnp.where(slots[None, :] == slot[:, None], weights[:, k][:, None], 0.0)
    return select, mix


BLOCK = 512
DOWN_SLOTS = 2
KERNEL_VMEM = 62 * 1024 * 1024


def section_kernel(
    dp_count, expert_count, per_expert,
    grouped, mix, in_cache, out_cache, w_up, w_down, mixed, other,
    up_buf, down_buf, arrived, hidden, part, returned,
    up_sem, down_sem, own_sem, there_send, there_recv, back_send, back_recv, back_own, cache_send, cache_recv,
):
    own_dp, own_expert = lax.axis_index("dp"), lax.axis_index("expert")
    me = own_dp * expert_count + own_expert
    tok_rows = mixed.shape[0]
    ups, downs = w_up.shape[1] // BLOCK, w_down.shape[1] // BLOCK

    def up_copy(f):
        columns = pl.ds(pl.multiple_of(f * BLOCK, BLOCK), BLOCK)
        return pltpu.make_async_copy(w_up.at[:, columns], up_buf.at[f], up_sem.at[f])

    def down_copy(n):
        columns = pl.ds(n * BLOCK, BLOCK)
        return pltpu.make_async_copy(w_down.at[:, columns], down_buf.at[n % DOWN_SLOTS], down_sem.at[n])

    half = expert_count // 2
    steps = sorted(
        ((de, dd) for de in range(expert_count) for dd in range(dp_count) if de or dd),
        key=lambda step: (abs(step[0] - half), step[1]),
    )

    def partner(de, dd):
        return lax.rem(own_dp + dd, dp_count), lax.rem(own_expert + de, expert_count)

    def rows_of(device):
        return pl.ds(pl.multiple_of(device * per_expert, per_expert), per_expert)

    barrier = pltpu.get_barrier_semaphore()
    for de, dd in steps:
        dp, expert = partner(de, dd)
        pl.semaphore_signal(
            barrier, inc=1, device_id={"dp": dp, "expert": expert}, device_id_type=pl.DeviceIdType.MESH
        )
    own_there = pltpu.make_async_copy(grouped.at[rows_of(me)], arrived.at[rows_of(me)], own_sem)
    own_there.start()
    pl.semaphore_wait(barrier, len(steps))

    sends = []
    for i, (de, dd) in enumerate(steps):
        dp, expert = partner(de, dd)
        sends.append(
            pltpu.make_async_remote_copy(
                src_ref=grouped.at[rows_of(dp * expert_count + expert)],
                dst_ref=arrived.at[rows_of(me)],
                send_sem=there_send.at[i],
                recv_sem=there_recv.at[i],
                device_id={"dp": dp, "expert": expert},
                device_id_type=pl.DeviceIdType.MESH,
            )
        )
        sends[-1].start()
    cache_copies = []
    for dd in range(1, dp_count):
        for c, cache in enumerate((out_cache, in_cache)):
            cache_copies.append(
                pltpu.make_async_remote_copy(
                    src_ref=cache,
                    dst_ref=other.at[dd - 1, c],
                    send_sem=cache_send.at[dd - 1, c],
                    recv_sem=cache_recv.at[dd - 1, c],
                    device_id={"dp": lax.rem(own_dp + dd, dp_count)},
                    device_id_type=pl.DeviceIdType.MESH,
                )
            )
            cache_copies[-1].start()

    @pl.loop(0, ups)
    def _(f):
        up_copy(f).start()

    for n in range(min(DOWN_SLOTS, downs)):
        down_copy(n).start()

    own_there.wait()
    for copy in sends:
        copy.wait()

    @pl.loop(0, ups)
    def _(f):
        up_copy(f).wait()
        value = jnp.dot(arrived[...], up_buf[f], preferred_element_type=jnp.float32)
        columns = pl.ds(pl.multiple_of(f * BLOCK, BLOCK), BLOCK)
        hidden[:, columns] = (value / (1.0 + jnp.exp(-value))).astype(jnp.bfloat16)

    backs = []
    for n in range(downs):
        columns = pl.ds(n * BLOCK, BLOCK)
        down_copy(n).wait()
        value = jnp.dot(hidden[...], down_buf[n % DOWN_SLOTS], preferred_element_type=jnp.float32)
        part[:, columns] = value.astype(jnp.bfloat16)
        if n + DOWN_SLOTS < downs:
            down_copy(n + DOWN_SLOTS).start()
        group = []
        for i, (de, dd) in enumerate(steps):
            dp, expert = partner(de, dd)
            group.append(
                pltpu.make_async_remote_copy(
                    src_ref=part.at[rows_of(dp * expert_count + expert), columns],
                    dst_ref=returned.at[rows_of(me), columns],
                    send_sem=back_send.at[n, i],
                    recv_sem=back_recv.at[n, i],
                    device_id={"dp": dp, "expert": expert},
                    device_id_type=pl.DeviceIdType.MESH,
                )
            )
            group[-1].start()
        group.append(
            pltpu.make_async_copy(part.at[rows_of(me), columns], returned.at[rows_of(me), columns], back_own.at[n])
        )
        group[-1].start()
        backs.append(group)

    for n in range(downs):
        columns = pl.ds(n * BLOCK, BLOCK)
        for copy in backs[n]:
            copy.wait()
        both = jnp.dot(mix[...], returned[:, columns], preferred_element_type=jnp.float32)
        mixed[:, columns] = both[:tok_rows] + both[tok_rows:]
    for copy in cache_copies:
        copy.wait()


def run_section_kernel(grouped, mix, in_cache, out_cache, w_up, w_down, per_expert):
    dp_count, expert_count = lax.axis_size("dp"), lax.axis_size("expert")
    tok_rows, width = in_cache.shape
    slots, units = grouped.shape[0], w_up.shape[1]
    peers = dp_count * expert_count - 1
    ups, downs = units // BLOCK, width // BLOCK
    vmem, anywhere = pl.BlockSpec(memory_space=pltpu.VMEM), pl.BlockSpec(memory_space=pl.ANY)
    dma = pltpu.SemaphoreType.DMA
    return pl.pallas_call(
        functools.partial(section_kernel, dp_count, expert_count, per_expert),
        out_shape=(
            jax.ShapeDtypeStruct((tok_rows, width), jnp.float32),
            jax.ShapeDtypeStruct((dp_count - 1, 2, tok_rows, width), jnp.bfloat16),
        ),
        in_specs=[vmem, vmem, anywhere, anywhere, anywhere, anywhere],
        out_specs=(vmem, anywhere),
        scratch_shapes=[
            pltpu.VMEM((ups, width, BLOCK), jnp.bfloat16),
            pltpu.VMEM((DOWN_SLOTS, units, BLOCK), jnp.bfloat16),
            pltpu.VMEM((slots, width), jnp.bfloat16),
            pltpu.VMEM((slots, units), jnp.bfloat16),
            pltpu.VMEM((slots, width), jnp.bfloat16),
            pltpu.VMEM((slots, width), jnp.bfloat16),
            dma((ups,)),
            dma((downs,)),
            dma,
            dma((peers,)),
            dma((peers,)),
            dma((downs, peers)),
            dma((downs, peers)),
            dma((downs,)),
            dma((dp_count - 1, 2)),
            dma((dp_count - 1, 2)),
        ],
        compiler_params=pltpu.CompilerParams(
            collective_id=0, has_side_effects=True, vmem_limit_bytes=KERNEL_VMEM
        ),
        cost_estimate=pl.CostEstimate(
            flops=4 * slots * width * units, bytes_accessed=4 * width * units, transcendentals=slots * units
        ),
    )(grouped, mix, in_cache, out_cache, w_up, w_down)


def fits_kernel(tok_rows, width, units, dp_count, group_size):
    slots = tok_rows * TOPK
    needed = 2 * (width * units + DOWN_SLOTS * units * BLOCK + slots * units + 8 * slots * width)
    whole = units % BLOCK == 0 and width % BLOCK == 0
    return group_size == EXPERTS and dp_count == 2 and whole and needed < KERNEL_VMEM


def own_part(sample_map, own_device, expert_count, tok_rows):
    dp_count = lax.axis_size("dp")
    ids = jnp.arange(sample_map.shape[0], dtype=jnp.int32)
    wanted = own_device * SAMP_DEV + jnp.arange(SAMP_DEV, dtype=jnp.int32)
    sources = jnp.sum(jnp.where(sample_map[None, :] == wanted[:, None], ids[None, :], 0), axis=1)
    back = lax.rem(lax.axis_index("dp") - sources // (SAMP_DEV * expert_count) + dp_count, dp_count)
    rows = jnp.arange(tok_rows, dtype=jnp.int32)
    row_source = jnp.repeat(sources % SAMP_DEV, ROWS) * ROWS + rows % ROWS
    row_back = jnp.repeat(back, ROWS)
    return [
        ((row_source[:, None] == rows[None, :]) & (row_back[:, None] == away)).astype(jnp.bfloat16)
        for away in range(dp_count)
    ]


def per_device(inputs, in_cache, out_cache, w_up, w_down, routing, gate_table, lengths, sample_map):
    tok_rows, width = inputs.shape[1:]
    dp_count = lax.axis_size("dp")
    expert_count = lax.axis_size("expert")
    group_size = dp_count * expert_count
    slice_count = group_size // EXPERTS
    own_dp = lax.axis_index("dp")
    own_device = own_dp * expert_count + lax.axis_index("expert")
    cap_slots = max(1, SAMP_DEV // dp_count)
    per_expert = tok_rows * TOPK // EXPERTS

    select, mix = token_plan(routing[0], gate_table[0], per_expert)
    grouped = jnp.dot(select, inputs[0], preferred_element_type=jnp.float32).astype(jnp.bfloat16)
    if fits_kernel(tok_rows, width, w_up.shape[2], dp_count, group_size):
        high = mix.astype(jnp.bfloat16)
        low = (mix - high.astype(jnp.float32)).astype(jnp.bfloat16)
        mixed, other = run_section_kernel(
            grouped, jnp.concatenate([high, low], axis=0), in_cache[0], out_cache[0], w_up[0], w_down[0], per_expert
        )
        picks = own_part(sample_map, own_device, expert_count, tok_rows)

        def moved(own, c):
            total = jnp.dot(picks[0], own, preferred_element_type=jnp.float32)
            for away in range(1, dp_count):
                total = total + jnp.dot(picks[away], other[away - 1, c], preferred_element_type=jnp.float32)
            return total.astype(jnp.bfloat16)

        out_moved, in_moved = moved(out_cache[0], 0), moved(in_cache[0], 1)
    else:
        grouped = grouped.reshape(EXPERTS, 1, per_expert, width)
        outgoing = jnp.broadcast_to(grouped, (EXPERTS, slice_count, per_expert, width)).reshape(
            group_size, per_expert, width
        )
        arrived = lax.all_to_all(outgoing, ("dp", "expert"), split_axis=0, concat_axis=0, tiled=True)

        to_send, arrival = cache_plan(sample_map, own_device, own_dp, dp_count, expert_count, cap_slots)
        send = jnp.concatenate(
            [
                in_cache[0].reshape(SAMP_DEV, 1, ROWS, width)[to_send],
                out_cache[0].reshape(SAMP_DEV, 1, ROWS, width)[to_send],
            ],
            axis=1,
        )
        send, arrived = lax.optimization_barrier((send, arrived))
        got = lax.all_to_all(send, "dp", split_axis=0, concat_axis=0, tiled=True)

        hidden = jax.nn.silu(
            jnp.dot(arrived.reshape(-1, width), w_up[0], preferred_element_type=jnp.float32)
        ).astype(jnp.bfloat16)
        partial_value = jnp.dot(hidden, w_down[0], preferred_element_type=jnp.float32).astype(jnp.bfloat16)
        returned = lax.all_to_all(
            partial_value.reshape(arrived.shape), ("dp", "expert"), split_axis=0, concat_axis=0, tiled=True
        ).reshape(-1, width)

        mix = jnp.broadcast_to(
            mix.reshape(tok_rows, EXPERTS, 1, per_expert), (tok_rows, EXPERTS, slice_count, per_expert)
        ).reshape(tok_rows, -1)
        high = mix.astype(jnp.bfloat16)
        low = (mix - high.astype(jnp.float32)).astype(jnp.bfloat16)
        both = jnp.dot(jnp.concatenate([high, low], axis=0), returned, preferred_element_type=jnp.float32)
        mixed = both[:tok_rows] + both[tok_rows:]

        in_moved = got[arrival, 0].reshape(tok_rows, width)
        out_moved = got[arrival, 1].reshape(tok_rows, width)

    row_numbers = jnp.arange(tok_rows, dtype=jnp.int32) % ROWS
    valid_rows = row_numbers < jnp.repeat(lengths, ROWS)
    delta_rows = jnp.where(
        valid_rows[:, None],
        (mixed - out_moved.astype(jnp.float32)).astype(jnp.bfloat16),
        jnp.zeros((), jnp.bfloat16),
    )
    new_out = (out_moved.astype(jnp.float32) + delta_rows.astype(jnp.float32)).astype(jnp.bfloat16)
    received = from_behind(delta_rows, "section", 1)
    next_input = (in_moved.astype(jnp.float32) + received.astype(jnp.float32)).astype(jnp.bfloat16)
    return (next_input[None], new_out[None])


def solution(mesh):
    split = P("section", ("dp", "expert"), None)
    placed = (split, split, split, P("section", None, ("dp", "expert")), split, split, split, P(("dp", "expert")), P())
    return jax.shard_map(per_device, mesh=mesh, in_specs=placed, out_specs=(split, split), check_vma=False)
```
